32 devices in a mesh: rep: 8 (over z, core), tp: 4 (over y, x).
Axes of the slice: x: 2, y: 2, z: 4, core: 2. Of those that a mesh axis runs over, the one named last changes fastest.
Arguments:
- hidden_state: bfloat16 [32, 3584], P('rep'), may hold values from -6 to 6
- lengths: int32 [32], P('rep'), may hold values from 1 to 2048, as said below
- old_qkv: bfloat16 [3584, 4608], P(None, 'tp'), may hold values from -0.09375 to 0.09375
- old_out: bfloat16 [3584, 3584], P(None, 'tp'), may hold values from -0.09375 to 0.09375
- cache_keys: bfloat16 [32, 2048, 512], P('rep', 'tp'), may hold values from -64 to 64
- cache_values: bfloat16 [32, 2048, 512], P('rep', 'tp'), may hold values from -6 to 6
- new_qkv: bfloat16 [3584, 4608], P(('rep', 'tp')), may hold values from -0.09375 to 0.09375
- new_out: bfloat16 [3584, 3584], P(('rep', 'tp')), may hold values from -0.09375 to 0.09375
Outputs:
- decoded: bfloat16 [32, 3584], P('rep', 'tp')
- resharded_qkv: bfloat16 [3584, 4608], P(None, 'tp')
- resharded_out: bfloat16 [3584, 3584], P(None, 'tp')
The draws below stay inside these ranges and needn't reach their ends.
Inputs may be any that keep to these rules, and one draw needn't show every extreme that they name: Every sequence has 1 to 2048 cached tokens, held in positions 0 to lengths - 1; in every draw some sequence fills its cache.
All inputs are finite; a program needn't handle non-finite values.
Results may differ from the reference program's by a relative error of at most 0.012.
Values may be sent and summed in bfloat16 or wider, within the bound.
No kernel may reach another device: no remote copies, remote signals or barrier semaphores. Data moves between devices by JAX's collectives and lax.ppermute only.
A program may use at most 128 MiB of HBM per device.

```python
import jax
import jax.numpy as jnp
from jax import lax

D = 3584
HQ = 28
KVH = 4
HD = 128
SEQS = 32
CACHE_LEN = 2048
COLS = 4608


def draw_lengths(key, part):
    drawn = jax.random.randint(key, (SEQS,), 1, CACHE_LEN + 1)
    chosen = jax.random.randint(jax.random.fold_in(key, 7), (), 0, SEQS)
    return jnp.where(jnp.arange(SEQS) == chosen, CACHE_LEN, drawn).astype(jnp.int32)


def draw_cache_keys(key, part):
    drawn = jax.random.normal(key, (SEQS, CACHE_LEN, KVH * HD), jnp.float32)
    return jnp.clip(drawn, -64.0, 64.0).astype(jnp.bfloat16)


def levels(rng, dims, pieces, least, largest):
    level = 1.0
    for axis_at, shards_of in pieces:
        steps = jax.random.uniform(jax.random.fold_in(jax.random.fold_in(rng, 6), axis_at), (shards_of,), jnp.float32, least / len(pieces), largest / len(pieces))
        level = level * jnp.repeat(jnp.exp(steps), dims[axis_at] // shards_of).reshape((-1,) + (1,) * (len(dims) - 1 - axis_at))
    return level


def bell_draw(stream_key, shape, deviation, bound, cuts=(), kind=jnp.bfloat16):
    values = deviation * jax.random.normal(stream_key, shape, jnp.float32)
    if cuts:
        values = values * levels(stream_key, shape, cuts, -0.22, 0.18)
    return jnp.clip(values, -bound, bound).astype(kind)


def setup_inputs(seed: int = 0) -> dict:
    splits = jax.random.split(jax.random.key(seed), 9)
    return {
        "hidden_state": bell_draw(splits[0], (SEQS, D), 1.0, 6.0, ((0, 8),)),
        "lengths": draw_lengths(jax.random.fold_in(splits[8], 71), 0),
        "old_qkv": bell_draw(splits[2], (D, COLS), D ** -0.5, 0.09375, ((1, 4),)),
        "old_out": bell_draw(splits[3], (HQ * HD, D), (HQ * HD) ** -0.5, 0.09375, ((1, 4),)),
        "cache_keys": draw_cache_keys(jax.random.fold_in(splits[8], 71), 0),
        "cache_values": bell_draw(splits[5], (SEQS, CACHE_LEN, KVH * HD), 1.0, 6.0, ((0, 8), (1, 4))),
        "new_qkv": bell_draw(splits[6], (D, COLS), D ** -0.5, 0.09375, ((0, 32),)),
        "new_out": bell_draw(splits[7], (HQ * HD, D), (HQ * HD) ** -0.5, 0.09375, ((0, 32),)),
    }


ROPE_BASE = 1000000.0

def rotate(vectors, positions):
    half_dim = vectors.shape[-1] // 2
    frequency = ROPE_BASE ** (-2.0 * jnp.arange(half_dim, dtype=jnp.float32) / (2 * half_dim))
    angles = positions.astype(jnp.float32)[:, None, None] * frequency
    first_half = vectors[..., :half_dim]
    second_half = vectors[..., half_dim:]
    return jnp.concatenate([first_half * jnp.cos(angles) - second_half * jnp.sin(angles), second_half * jnp.cos(angles) + first_half * jnp.sin(angles)], axis=-1)

def reference(hidden_state, lengths, old_qkv, old_out, cache_keys, cache_values, new_qkv, new_out):
    joined = jnp.dot(hidden_state, old_qkv, preferred_element_type=jnp.float32).astype(jnp.bfloat16)
    q_width = HQ * HD
    k_width = KVH * HD
    queries = rotate(joined[:, :q_width].astype(jnp.float32).reshape(SEQS, HQ, HD), lengths).astype(jnp.bfloat16)
    own_keys = rotate(joined[:, q_width:q_width + k_width].astype(jnp.float32).reshape(SEQS, KVH, HD), lengths).astype(jnp.bfloat16)
    own_values = joined[:, q_width + k_width:].reshape(SEQS, KVH, HD)
    group_size = HQ // KVH
    inv_root = 1.0 / jnp.sqrt(jnp.float32(HD))

    def attend(per_sequence):
        query_row, own_key, own_value, length, seq_keys, seq_values = per_sequence
        grouped = query_row.reshape(KVH, group_size, HD).astype(jnp.float32)
        key_blocks = seq_keys.reshape(CACHE_LEN, KVH, HD).astype(jnp.float32)
        value_blocks = seq_values.reshape(CACHE_LEN, KVH, HD).astype(jnp.float32)
        scores = jnp.einsum('kgd,tkd->kgt', grouped, key_blocks) * inv_root
        live_mask = jnp.arange(CACHE_LEN, dtype=jnp.int32) < length
        scores = jnp.where(live_mask, scores, jnp.float32(-1e+30))
        own_score = lax.optimization_barrier(jnp.sum(grouped * own_key.astype(jnp.float32)[:, None, :], axis=-1)) * inv_root
        top_score = jnp.maximum(lax.optimization_barrier(jnp.max(scores, axis=-1)), own_score)
        weights = jnp.where(live_mask, jnp.exp(scores - top_score[..., None]), jnp.float32(0.0)).astype(jnp.bfloat16)
        own_weight = lax.optimization_barrier(jnp.exp(own_score - top_score).astype(jnp.bfloat16)).astype(jnp.float32)
        numerator = jnp.einsum('kgt,tkd->kgd', weights.astype(jnp.float32), value_blocks)
        numerator = numerator + own_weight[..., None] * own_value.astype(jnp.float32)[:, None, :]
        denominator = lax.optimization_barrier(jnp.sum(weights.astype(jnp.float32), axis=-1)) + own_weight
        return (numerator / denominator[..., None]).reshape(HQ * HD).astype(jnp.bfloat16)
    attended = lax.map(attend, (queries, own_keys, own_values, lengths, cache_keys, cache_values))
    decoded = jnp.dot(attended, old_out, preferred_element_type=jnp.float32).astype(jnp.bfloat16)
    return (decoded, new_qkv, new_out)
```

```python
import jax
import jax.numpy as jnp
from jax import lax
from jax.experimental import pallas as pl
from jax.experimental.pallas import tpu as pltpu
from jax.sharding import Mesh
from jax.sharding import PartitionSpec as P


HQ = 28
KVH = 4
HD = 128
CORES = 2

ROPE_BASE = 1000000.0


def rotate(vectors, positions):
    half_dim = vectors.shape[-1] // 2
    frequency = ROPE_BASE ** (-2.0 * jnp.arange(half_dim, dtype=jnp.float32) / (2 * half_dim))
    angles = positions.astype(jnp.float32)[:, None, None] * frequency
    first_half = vectors[..., :half_dim]
    second_half = vectors[..., half_dim:]
    return jnp.concatenate(
        [
            first_half * jnp.cos(angles) - second_half * jnp.sin(angles),
            second_half * jnp.cos(angles) + first_half * jnp.sin(angles),
        ],
        axis=-1,
    )


def place_pieces(device, pieces, row_of, outs, widths, total_rows):
    count = len(pieces)
    height = pieces[0].shape[0]
    aliased = 0 if outs is None else len(outs)

    def kernel(device_ref, *refs):
        piece_refs = refs[:count]
        out_refs = refs[count + aliased : count + aliased + len(widths)]
        sem = refs[-1]
        copies = []
        for at, piece in enumerate(piece_refs):
            first = pl.multiple_of(row_of[at](device_ref[0]), 16)
            column = 0
            for out_at, (out, width) in enumerate(zip(out_refs, widths)):
                copies.append(
                    pltpu.make_async_copy(
                        piece.at[:, pl.ds(column, width)],
                        out.at[pl.ds(first, height), :],
                        sem.at[at, out_at],
                    )
                )
                column += width
        for copy in copies:
            copy.start()
        for copy in copies:
            copy.wait()

    dtype = pieces[0].dtype
    return pl.pallas_call(
        kernel,
        out_shape=[jax.ShapeDtypeStruct((total_rows, width), dtype) for width in widths],
        in_specs=[pl.BlockSpec(memory_space=pltpu.SMEM)]
        + [pl.BlockSpec(memory_space=pl.ANY)] * (count + aliased),
        out_specs=[pl.BlockSpec(memory_space=pl.ANY)] * len(widths),
        scratch_shapes=[pltpu.SemaphoreType.DMA((count, len(widths)))],
        input_output_aliases={1 + count + at: at for at in range(aliased)},
    )(device, *pieces, *(() if outs is None else outs))


def reshard_by_permutes(new_qkv, new_out, outer, tp):
    height = new_qkv.shape[0]
    widths = (new_qkv.shape[1] // tp, new_out.shape[1] // tp)
    t = lax.axis_index("tp")
    device = lax.axis_index(("outer", "core", "tp")).astype(jnp.int32).reshape(1)
    ring = [(i, (i + 1) % outer) for i in range(outer)]
    swap = [(i, i ^ 1) for i in range(CORES)]

    def columns_for(peer):
        return jnp.concatenate(
            [
                lax.dynamic_slice_in_dim(array, peer * width, width, 1)
                for array, width in zip((new_qkv, new_out), widths)
            ],
            axis=1,
        )

    mine = {}
    for j in range(tp):
        mine[0, j] = columns_for(t ^ j)
        if j:
            mine[0, j] = lax.ppermute(mine[0, j], "tp", [(i, i ^ j) for i in range(tp)])
    for s in range(1, outer):
        for j in range(tp):
            mine[s, j] = lax.ppermute(mine[s - 1, j], "outer", ring)
    theirs = {}
    for at, piece in mine.items():
        theirs[at] = lax.ppermute(piece, "core", swap)

    def row_of(at, other):
        def rows(device):
            z = device // (CORES * tp)
            c = device // tp % CORES
            z = (z - at[0] + outer) % outer
            c = 1 - c if other else c
            return ((z * CORES + c) * tp + (device % tp ^ at[1])) * height

        return rows

    outs = None
    for group in place_groups(outer, tp):
        pieces = [mine[at] for at in group] + [theirs[at] for at in group]
        rows = [row_of(at, False) for at in group] + [row_of(at, True) for at in group]
        outs = place_pieces(device, pieces, rows, outs, widths, height * outer * CORES * tp)
    return tuple(outs)


def place_groups(outer, tp):
    blocks = [(s, j) for s in range(outer) for j in range(tp)]
    last = blocks[-1:]
    return [
        [at for at in blocks if at[0] < outer - 2],
        [at for at in blocks if at[0] == outer - 2],
        [at for at in blocks if at[0] == outer - 1 and at not in last],
        last,
    ]


def reshard_by_collectives(new_qkv, new_out):
    return tuple(
        lax.all_gather(
            lax.all_to_all(array, "tp", split_axis=1, concat_axis=0, tiled=True),
            ("outer", "core"),
            axis=0,
            tiled=True,
        )
        for array in (new_qkv, new_out)
    )


def decode(hidden_state, lengths, old_qkv, old_out, cache_keys, cache_values):
    seq_count = hidden_state.shape[0]
    local_joined = jnp.dot(hidden_state, old_qkv, preferred_element_type=jnp.float32).astype(
        jnp.bfloat16
    )
    joined_rows = lax.all_gather(local_joined, "tp", axis=1, tiled=True)
    q_width = HQ * HD
    k_width = KVH * HD
    group_size = HQ // KVH
    queries = rotate(
        joined_rows[:, :q_width].astype(jnp.float32).reshape(seq_count, HQ, HD), lengths
    ).astype(jnp.bfloat16)
    own_keys = rotate(
        joined_rows[:, q_width : q_width + k_width].astype(jnp.float32).reshape(seq_count, KVH, HD),
        lengths,
    ).astype(jnp.bfloat16)
    own_values = joined_rows[:, q_width + k_width :].reshape(seq_count, KVH, HD)
    inv_root = 1.0 / jnp.sqrt(jnp.float32(HD))
    cache_rows = cache_keys.shape[1]
    grouped = queries.reshape(seq_count, KVH, group_size, HD)
    key_blocks = cache_keys.reshape(seq_count, cache_rows, KVH, HD)
    value_blocks = cache_values.reshape(seq_count, cache_rows, KVH, HD)
    scores = (
        jnp.einsum("skgd,stkd->skgt", grouped, key_blocks, preferred_element_type=jnp.float32)
        * inv_root
    )
    positions = lax.axis_index("tp") * cache_rows + jnp.arange(cache_rows, dtype=jnp.int32)
    live_mask = (positions[None, :] < lengths[:, None])[:, None, None, :]
    scores = jnp.where(live_mask, scores, jnp.float32(-1e30))
    own_score = (
        jnp.sum(grouped.astype(jnp.float32) * own_keys.astype(jnp.float32)[:, :, None, :], axis=-1)
        * inv_root
    )
    local_top = jnp.maximum(jnp.max(scores, axis=-1), own_score)
    top_score = lax.pmax(local_top, "tp")
    weights = jnp.where(live_mask, jnp.exp(scores - top_score[..., None]), jnp.float32(0.0)).astype(
        jnp.bfloat16
    )
    numer_part = jnp.einsum(
        "skgt,stkd->skgd", weights, value_blocks, preferred_element_type=jnp.float32
    )
    denom_part = jnp.sum(weights.astype(jnp.float32), axis=-1)
    numerator, denominator = lax.psum((numer_part, denom_part), "tp")
    own_weight = lax.optimization_barrier(
        jnp.exp(own_score - top_score).astype(jnp.bfloat16)
    ).astype(jnp.float32)
    numerator = numerator + own_weight[..., None] * own_values.astype(jnp.float32)[:, :, None, :]
    denominator = denominator + own_weight
    attended = (numerator / denominator[..., None]).reshape(seq_count, q_width).astype(jnp.bfloat16)
    return jnp.dot(attended, old_out, preferred_element_type=jnp.float32).astype(jnp.bfloat16)


def solution(mesh):
    rep, tp = mesh.shape["rep"], mesh.shape["tp"]
    outer = rep // CORES
    split = Mesh(mesh.devices.reshape(outer, CORES, tp), ("outer", "core", "tp"))
    rep_axes = ("outer", "core")

    def by_permutes(hidden_state, lengths, old_qkv, old_out, cache_keys, cache_values, new_qkv, new_out):
        weights = reshard_by_permutes(new_qkv, new_out, outer, tp)
        decoded = decode(hidden_state, lengths, old_qkv, old_out, cache_keys, cache_values)
        return (decoded, *weights)

    def by_collectives(hidden_state, lengths, old_qkv, old_out, cache_keys, cache_values, new_qkv, new_out):
        weights = reshard_by_collectives(new_qkv, new_out)
        decoded = decode(hidden_state, lengths, old_qkv, old_out, cache_keys, cache_values)
        return (decoded, *weights)

    in_specs = (
        P(rep_axes, None),
        P(rep_axes),
        P(None, "tp"),
        P(None, "tp"),
        P(rep_axes, "tp", None),
        P(rep_axes, "tp", None),
        P((*rep_axes, "tp"), None),
        P((*rep_axes, "tp"), None),
    )
    out_specs = (P(rep_axes, "tp"), P(None, "tp"), P(None, "tp"))

    def step(*args):
        new_qkv, new_out = args[-2:]
        height = new_qkv.shape[0] // (rep * tp)
        widths = (new_qkv.shape[1] // tp, new_out.shape[1] // tp)
        pieced = height % 16 == 0 and all(width % 128 == 0 for width in widths)
        body = by_permutes if pieced and outer >= 4 else by_collectives
        run = jax.shard_map(
            body, mesh=split, in_specs=in_specs, out_specs=out_specs, check_vma=False
        )
        return run(*args)

    return step
```

```python
import jax
import jax.numpy as jnp
from jax import lax
from jax.experimental import pallas as pl
from jax.experimental.pallas import tpu as pltpu
from jax.sharding import Mesh
from jax.sharding import PartitionSpec as P


HQ = 28
KVH = 4
HD = 128
CORES = 2

ROPE_BASE = 1000000.0


def rotate(vectors, positions):
    half_dim = vectors.shape[-1] // 2
    frequency = ROPE_BASE ** (-2.0 * jnp.arange(half_dim, dtype=jnp.float32) / (2 * half_dim))
    angles = positions.astype(jnp.float32)[:, None, None] * frequency
    first_half = vectors[..., :half_dim]
    second_half = vectors[..., half_dim:]
    return jnp.concatenate(
        [
            first_half * jnp.cos(angles) - second_half * jnp.sin(angles),
            second_half * jnp.cos(angles) + first_half * jnp.sin(angles),
        ],
        axis=-1,
    )


def place_pieces(device, pieces, row_of, outs, widths, total_rows):
    count = len(pieces)
    height = pieces[0].shape[0]
    aliased = 0 if outs is None else len(outs)

    def kernel(device_ref, *refs):
        piece_refs = refs[:count]
        out_refs = refs[count + aliased : count + aliased + len(widths)]
        sem = refs[-1]
        copies = []
        for at, piece in enumerate(piece_refs):
            first = pl.multiple_of(row_of[at](device_ref[0]), 16)
            column = 0
            for out_at, (out, width) in enumerate(zip(out_refs, widths)):
                copies.append(
                    pltpu.make_async_copy(
                        piece.at[:, pl.ds(column, width)],
                        out.at[pl.ds(first, height), :],
                        sem.at[at, out_at],
                    )
                )
                column += width
        for copy in copies:
            copy.start()
        for copy in copies:
            copy.wait()

    dtype = pieces[0].dtype
    return pl.pallas_call(
        kernel,
        out_shape=[jax.ShapeDtypeStruct((total_rows, width), dtype) for width in widths],
        in_specs=[pl.BlockSpec(memory_space=pltpu.SMEM)]
        + [pl.BlockSpec(memory_space=pltpu.VMEM)] * count
        + [pl.BlockSpec(memory_space=pl.ANY)] * aliased,
        out_specs=[pl.BlockSpec(memory_space=pl.ANY)] * len(widths),
        scratch_shapes=[pltpu.SemaphoreType.DMA((count, len(widths)))],
        input_output_aliases={1 + count + at: at for at in range(aliased)},
        compiler_params=pltpu.CompilerParams(
            vmem_limit_bytes=count * pieces[0].size * dtype.itemsize + (2 << 20)
        ),
    )(device, *pieces, *(() if outs is None else outs))


def reshard_by_permutes(new_qkv, new_out, outer, tp):
    height = new_qkv.shape[0]
    widths = (new_qkv.shape[1] // tp, new_out.shape[1] // tp)
    t = lax.axis_index("tp")
    device = lax.axis_index(("outer", "core", "tp")).astype(jnp.int32).reshape(1)
    ring = [(i, (i + 1) % outer) for i in range(outer)]
    swap = [(i, i ^ 1) for i in range(CORES)]

    def columns_for(peer):
        return jnp.concatenate(
            [
                lax.dynamic_slice_in_dim(array, peer * width, width, 1)
                for array, width in zip((new_qkv, new_out), widths)
            ],
            axis=1,
        )

    mine = {}
    for j in range(tp):
        mine[0, j] = columns_for(t ^ j)
        if j:
            mine[0, j] = lax.ppermute(mine[0, j], "tp", [(i, i ^ j) for i in range(tp)])
    for s in range(1, outer):
        for j in range(tp):
            mine[s, j] = lax.ppermute(mine[s - 1, j], "outer", ring)
    theirs = {}
    for at, piece in mine.items():
        theirs[at] = lax.ppermute(piece, "core", swap)

    def row_of(at, other):
        def rows(device):
            z = device // (CORES * tp)
            c = device // tp % CORES
            z = (z - at[0] + outer) % outer
            c = 1 - c if other else c
            return ((z * CORES + c) * tp + (device % tp ^ at[1])) * height

        return rows

    outs = None
    for group in place_groups(outer, tp):
        pieces = [mine[at] for at in group] + [theirs[at] for at in group]
        rows = [row_of(at, False) for at in group] + [row_of(at, True) for at in group]
        outs = place_pieces(device, pieces, rows, outs, widths, height * outer * CORES * tp)
    return tuple(outs)


def place_groups(outer, tp):
    blocks = [(s, j) for s in range(outer) for j in range(tp)]
    last = blocks[-1:]
    return [
        [at for at in blocks if at[0] < outer - 2],
        [at for at in blocks if at[0] == outer - 2],
        [at for at in blocks if at[0] == outer - 1 and at not in last],
        last,
    ]


def reshard_by_collectives(new_qkv, new_out):
    return tuple(
        lax.all_gather(
            lax.all_to_all(array, "tp", split_axis=1, concat_axis=0, tiled=True),
            ("outer", "core"),
            axis=0,
            tiled=True,
        )
        for array in (new_qkv, new_out)
    )


def decode(hidden_state, lengths, old_qkv, old_out, cache_keys, cache_values):
    seq_count = hidden_state.shape[0]
    local_joined = jnp.dot(hidden_state, old_qkv, preferred_element_type=jnp.float32).astype(
        jnp.bfloat16
    )
    joined_rows = lax.all_gather(local_joined, "tp", axis=1, tiled=True)
    q_width = HQ * HD
    k_width = KVH * HD
    group_size = HQ // KVH
    queries = rotate(
        joined_rows[:, :q_width].astype(jnp.float32).reshape(seq_count, HQ, HD), lengths
    ).astype(jnp.bfloat16)
    own_keys = rotate(
        joined_rows[:, q_width : q_width + k_width].astype(jnp.float32).reshape(seq_count, KVH, HD),
        lengths,
    ).astype(jnp.bfloat16)
    own_values = joined_rows[:, q_width + k_width :].reshape(seq_count, KVH, HD)
    inv_root = 1.0 / jnp.sqrt(jnp.float32(HD))
    cache_rows = cache_keys.shape[1]
    grouped = queries.reshape(seq_count, KVH, group_size, HD)
    key_blocks = cache_keys.reshape(seq_count, cache_rows, KVH, HD)
    value_blocks = cache_values.reshape(seq_count, cache_rows, KVH, HD)
    scores = (
        jnp.einsum("skgd,stkd->skgt", grouped, key_blocks, preferred_element_type=jnp.float32)
        * inv_root
    )
    positions = lax.axis_index("tp") * cache_rows + jnp.arange(cache_rows, dtype=jnp.int32)
    live_mask = (positions[None, :] < lengths[:, None])[:, None, None, :]
    scores = jnp.where(live_mask, scores, jnp.float32(-1e30))
    own_score = (
        jnp.sum(grouped.astype(jnp.float32) * own_keys.astype(jnp.float32)[:, :, None, :], axis=-1)
        * inv_root
    )
    local_top = jnp.maximum(jnp.max(scores, axis=-1), own_score)
    top_score = lax.pmax(local_top, "tp")
    weights = jnp.where(live_mask, jnp.exp(scores - top_score[..., None]), jnp.float32(0.0)).astype(
        jnp.bfloat16
    )
    numer_part = jnp.einsum(
        "skgt,stkd->skgd", weights, value_blocks, preferred_element_type=jnp.float32
    )
    denom_part = jnp.sum(weights.astype(jnp.float32), axis=-1)
    numerator, denominator = lax.psum((numer_part, denom_part), "tp")
    own_weight = lax.optimization_barrier(
        jnp.exp(own_score - top_score).astype(jnp.bfloat16)
    ).astype(jnp.float32)
    numerator = numerator + own_weight[..., None] * own_values.astype(jnp.float32)[:, :, None, :]
    denominator = denominator + own_weight
    attended = (numerator / denominator[..., None]).reshape(seq_count, q_width).astype(jnp.bfloat16)
    return jnp.dot(attended, old_out, preferred_element_type=jnp.float32).astype(jnp.bfloat16)


def solution(mesh):
    rep, tp = mesh.shape["rep"], mesh.shape["tp"]
    outer = rep // CORES
    split = Mesh(mesh.devices.reshape(outer, CORES, tp), ("outer", "core", "tp"))
    rep_axes = ("outer", "core")

    def by_permutes(hidden_state, lengths, old_qkv, old_out, cache_keys, cache_values, new_qkv, new_out):
        weights = reshard_by_permutes(new_qkv, new_out, outer, tp)
        decoded = decode(hidden_state, lengths, old_qkv, old_out, cache_keys, cache_values)
        return (decoded, *weights)

    def by_collectives(hidden_state, lengths, old_qkv, old_out, cache_keys, cache_values, new_qkv, new_out):
        weights = reshard_by_collectives(new_qkv, new_out)
        decoded = decode(hidden_state, lengths, old_qkv, old_out, cache_keys, cache_values)
        return (decoded, *weights)

    in_specs = (
        P(rep_axes, None),
        P(rep_axes),
        P(None, "tp"),
        P(None, "tp"),
        P(rep_axes, "tp", None),
        P(rep_axes, "tp", None),
        P((*rep_axes, "tp"), None),
        P((*rep_axes, "tp"), None),
    )
    out_specs = (P(rep_axes, "tp"), P(None, "tp"), P(None, "tp"))

    def step(*args):
        new_qkv, new_out = args[-2:]
        height = new_qkv.shape[0] // (rep * tp)
        widths = (new_qkv.shape[1] // tp, new_out.shape[1] // tp)
        pieced = height % 16 == 0 and all(width % 128 == 0 for width in widths)
        body = by_permutes if pieced and outer >= 4 else by_collectives
        run = jax.shard_map(
            body, mesh=split, in_specs=in_specs, out_specs=out_specs, check_vma=False
        )
        return run(*args)

    return step
```
